32 devices in a mesh: ctx: 16 (over z, x, core), head: 2 (over y).
Axes of the slice: x: 2, y: 2, z: 4, core: 2. Of those that a mesh axis runs over, the one named last changes fastest.
Arguments:
- queries: bfloat16 [256, 4096], P('ctx', 'head'), may hold values from -1500 to 1500
- cache_keys: bfloat16 [65536, 2048], P('ctx', 'head'), may hold values from -15 to 15
- prefix_cache_values: bfloat16 [65536, 2048], P('ctx', 'head'), may hold values from -6 to 6
- incoming_keys: bfloat16 [256, 2048], P('ctx', 'head'), may hold values from -15 to 15
- incoming_values: bfloat16 [256, 2048], P('ctx', 'head'), may hold values from -6 to 6
Outputs:
- attended: bfloat16 [256, 4096], P('ctx', 'head')
The draws below stay inside these ranges and needn't reach their ends.
All inputs are finite; a program needn't handle non-finite values.
Results may differ from the reference program's by a relative error of at most 0.005.
Values may be sent and summed in bfloat16 or wider, within the bound.
A program may use at most 64 MiB of HBM per device.

```python
import jax
import jax.numpy as jnp
from jax import lax

QUERY_HEAD_COUNT = 32
KEY_VALUE_HEADS = 16
HEAD_SIZE = 128
PREFIX_TOKENS = 65536
NEW_TOKEN_COUNT = 256


def chosen_pairs(key):
    picker = jax.random.fold_in(key, 12)
    first = jax.random.randint(jax.random.fold_in(picker, 1), (16,), 0, PREFIX_TOKENS)
    second = (first + PREFIX_TOKENS // 2) % PREFIX_TOKENS
    query_rows = jax.random.randint(jax.random.fold_in(picker, 2), (16,), 0, NEW_TOKEN_COUNT)
    current_query_head = jax.random.randint(jax.random.fold_in(picker, 3), (16,), 0, QUERY_HEAD_COUNT)
    strength = jax.random.uniform(jax.random.fold_in(picker, 4), (16,), jnp.float32, 1.8, 4.5)
    return (first, second, query_rows, current_query_head, strength)


def base_keys(key):
    sampled_inputs = 2.5 * jax.random.truncated_normal(jax.random.fold_in(key, 11), -6.0, 6.0, (PREFIX_TOKENS, KEY_VALUE_HEADS * HEAD_SIZE), jnp.float32)
    first, second, query_rows, current_query_head, strength = chosen_pairs(key)
    sampled_inputs = sampled_inputs.at[second].set(0.99 * sampled_inputs[first])
    return sampled_inputs


def draw_cache_keys(key, part):
    return base_keys(key).astype(jnp.bfloat16)


def draw_queries(key, part):
    sampled_inputs = jax.random.truncated_normal(jax.random.fold_in(key, 13), -6.0, 6.0, (NEW_TOKEN_COUNT, QUERY_HEAD_COUNT * HEAD_SIZE), jnp.float32)
    key_table = base_keys(key).astype(jnp.bfloat16).astype(jnp.float32)
    first, second, query_rows, current_query_head, strength = chosen_pairs(key)
    key_value_head = current_query_head // (QUERY_HEAD_COUNT // KEY_VALUE_HEADS)
    offsets = jnp.arange(HEAD_SIZE, dtype=jnp.int32)
    key_cols = key_value_head[:, None] * HEAD_SIZE + offsets[None, :]
    picked = key_table[first[:, None], key_cols] * strength[:, None]
    query_cols = current_query_head[:, None] * HEAD_SIZE + offsets[None, :]
    sampled_inputs = sampled_inputs.at[query_rows[:, None], query_cols].set(picked)
    return sampled_inputs.astype(jnp.bfloat16)


def levels(own_key, dims, shards, least, largest):
    gain, own = 1.0, jax.random.fold_in(own_key, 6)
    for dim, parts in shards:
        steps = jnp.exp(jax.random.uniform(jax.random.fold_in(own, dim), (parts,), jnp.float32, least / len(shards), largest / len(shards)))
        gain = gain * jnp.repeat(steps, dims[dim] // parts).reshape([-1 if axis == dim else 1 for axis in range(len(dims))])
    return gain


def scatter_about(rng, extent, spread, bound, shards=(), kind=jnp.bfloat16):
    drawn = jax.random.normal(rng, extent, jnp.float32) * spread
    if len(shards) > 0:
        drawn = levels(rng, extent, shards, -0.22, 0.18) * drawn
    return jnp.clip(drawn, min=-bound, max=bound).astype(kind)


def setup_inputs(seed: int = 0) -> dict:
    splits = jax.random.split(jax.random.key(seed), 6)
    return {
        "queries": draw_queries(jax.random.fold_in(splits[5], 71), 0),
        "cache_keys": draw_cache_keys(jax.random.fold_in(splits[5], 71), 0),
        "prefix_cache_values": scatter_about(splits[2], (PREFIX_TOKENS, KEY_VALUE_HEADS * HEAD_SIZE), 1.0, 6.0, ((0, 16), (1, 2))),
        "incoming_keys": scatter_about(splits[3], (NEW_TOKEN_COUNT, KEY_VALUE_HEADS * HEAD_SIZE), 2.5, 15.0, ((0, 16), (1, 2))),
        "incoming_values": scatter_about(splits[4], (NEW_TOKEN_COUNT, KEY_VALUE_HEADS * HEAD_SIZE), 1.0, 6.0, ((0, 16), (1, 2))),
    }


score_scale = 168.0 ** -0.5


def prefix_step(state, key_block, query_heads):
    out_acc, row_max, row_sum = state
    block_keys, block_values = key_block
    scores = jnp.einsum("gqd,kd->gqk", query_heads.astype(jnp.float32), block_keys.astype(jnp.float32)) * score_scale
    new_max = jnp.maximum(row_max, jnp.max(scores, axis=-1))
    decay = jnp.exp(row_max - new_max)
    probs = jnp.exp(scores - new_max[..., None])
    row_sum = row_sum * decay + jnp.sum(probs, axis=-1)
    rounded = lax.optimization_barrier(probs.astype(jnp.bfloat16)).astype(jnp.float32)
    out_acc = out_acc * decay[..., None] + jnp.einsum("gqk,kd->gqd", rounded, block_values.astype(jnp.float32))
    return (out_acc, new_max, row_sum), None


def one_head(operands):
    query_heads, head_keys, head_values, fresh_keys, fresh_values = operands
    group_size, total_rows, _ = query_heads.shape
    block_size = min(512, head_keys.shape[0])
    count = head_keys.shape[0] // block_size
    blocks = (head_keys.reshape(count, block_size, HEAD_SIZE), head_values.reshape(count, block_size, HEAD_SIZE))
    init = (jnp.zeros((group_size, total_rows, HEAD_SIZE), jnp.float32),
            jnp.full((group_size, total_rows), -1e30, jnp.float32),
            jnp.zeros((group_size, total_rows), jnp.float32))
    (out_acc, row_max, row_sum), _ = lax.scan(lambda state, key_block: prefix_step(state, key_block, query_heads), init, blocks)
    scores = jnp.einsum("gqd,kd->gqk", query_heads.astype(jnp.float32), fresh_keys.astype(jnp.float32)) * score_scale
    positions = jnp.arange(total_rows, dtype=jnp.int32)
    causal_mask = positions[None, :] <= positions[:, None]
    scores = jnp.where(causal_mask[None], scores, -1e30)
    fresh_max = jnp.max(scores, axis=-1)
    fresh_probs = jnp.where(causal_mask[None], jnp.exp(scores - fresh_max[..., None]), 0.0)
    fresh_sum = jnp.sum(fresh_probs, axis=-1)
    rounded = lax.optimization_barrier(fresh_probs.astype(jnp.bfloat16)).astype(jnp.float32)
    fresh_out = jnp.einsum("gqk,kd->gqd", rounded, fresh_values.astype(jnp.float32))
    merged_max = jnp.maximum(row_max, fresh_max)
    old_weight = jnp.exp(row_max - merged_max)
    new_weight = jnp.exp(fresh_max - merged_max)
    numer = out_acc * old_weight[..., None] + fresh_out * new_weight[..., None]
    denom = row_sum * old_weight + fresh_sum * new_weight
    return (numer / denom[..., None]).astype(jnp.bfloat16)


def reference(queries, cache_keys, prefix_cache_values, incoming_keys, incoming_values):
    total_rows = queries.shape[0]
    kv_heads = cache_keys.shape[1] // HEAD_SIZE
    group_size = queries.shape[1] // cache_keys.shape[1]
    query_heads = queries.reshape(total_rows, kv_heads, group_size, HEAD_SIZE).transpose(1, 2, 0, 3)
    head_keys = cache_keys.reshape(-1, kv_heads, HEAD_SIZE).transpose(1, 0, 2)
    head_values = prefix_cache_values.reshape(-1, kv_heads, HEAD_SIZE).transpose(1, 0, 2)
    fresh_keys = incoming_keys.reshape(total_rows, kv_heads, HEAD_SIZE).transpose(1, 0, 2)
    fresh_values = incoming_values.reshape(total_rows, kv_heads, HEAD_SIZE).transpose(1, 0, 2)
    outputs = lax.map(one_head, (query_heads, head_keys, head_values, fresh_keys, fresh_values))
    return outputs.transpose(2, 0, 1, 3).reshape(total_rows, -1)
```

```python
import functools
import math

import jax
import jax.numpy as jnp
from jax import lax
from jax.experimental import pallas as pl
from jax.experimental.pallas import tpu as pltpu
from jax.sharding import PartitionSpec as P

HEAD_SIZE = 128
LANES = 128
SUBLANES = 8
SUM_ROW = 4
TILE_ROWS = 256
BLOCK_KEYS = 1024
PIECE_KEYS = 256
EXP2_SCALE = 168.0 ** (-0.5) * math.log2(math.e)
MASKED = -1e30
BF16, F32 = jnp.bfloat16, jnp.float32


def nt_dot(a, b):
    return lax.dot_general(a, b, (((1,), (1,)), ((), ())), preferred_element_type=F32)


def tn_dot(a, b):
    return lax.dot_general(a, b, (((0,), (0,)), ((), ())), preferred_element_type=F32)


def fold(x, op):
    parts = [x[i] for i in range(x.shape[0])]
    while len(parts) > 1:
        parts = [op(*parts[i:i + 2]) if i + 1 < len(parts) else parts[i] for i in range(0, len(parts), 2)]
    return parts[0]


def kernel(
    devices, heads, group, own, block,
    q_hbm, k_hbm, v_hbm, fk_hbm, fv_hbm, out_ref,
    qown, qbuf, kbuf, vbuf, fkbuf, fvbuf, scores_even, scores_odd, fresh_scores, relative,
    block_max, row_max, row_sum, acc, obuf, xbuf, sbuf, mbuf, rbuf, rmbuf,
    q_sem, k_sem, v_sem, f_sem, gather_send, gather_recv, relay_send, relay_recv,
    x_send, x_recv, o_send, o_recv, m_send, m_recv,
):
    pairs = devices // 2
    each = group * own
    tile_pairs = qbuf.shape[3]
    tiles = qbuf.shape[1]
    rows = 2 * tile_pairs * each
    blocks = kbuf.shape[1] // block
    units = heads * tiles
    early = heads // 2 if tiles > 1 else heads
    me = lax.axis_index("ctx")
    core, pair = lax.rem(me, 2), lax.div(me, 2)
    my_tile, my_place = lax.div(pair, tile_pairs), lax.rem(pair, tile_pairs)

    def unit(u):
        far = u - early
        late = u - heads * (tiles - 1)
        is_early, is_late = u < early, u >= early + heads * (tiles - 1)
        far_step, far_head = 1 + lax.div(jnp.maximum(far, 0), heads), lax.rem(jnp.maximum(far, 0), heads)
        step = jnp.where(is_early | is_late, 0, far_step)
        h = jnp.where(is_early, u, jnp.where(is_late, late, far_head))
        return h, step, lax.rem(my_tile + step, tiles)

    def head_columns(h):
        return pl.ds(pl.multiple_of(h * HEAD_SIZE, HEAD_SIZE), HEAD_SIZE)

    def q_copy(h, g):
        columns = pl.ds((h * group + g) * HEAD_SIZE, HEAD_SIZE)
        return pltpu.make_async_copy(q_hbm.at[:, columns], qown.at[h, pl.ds(g * own, own)], q_sem.at[h, g])

    def q_place(h, g):
        columns = pl.ds((h * group + g) * HEAD_SIZE, HEAD_SIZE)
        return pltpu.make_async_copy(
            q_hbm.at[:, columns], qbuf.at[h, my_tile, core, my_place, pl.ds(g * own, own)],
            gather_recv.at[h, my_tile],
        )

    def k_copy(h):
        return pltpu.make_async_copy(k_hbm.at[:, head_columns(h)], kbuf.at[h], k_sem.at[h])

    def v_copy(h):
        return pltpu.make_async_copy(v_hbm.at[:, head_columns(h)], vbuf.at[h], v_sem.at[h])

    fk_copy = pltpu.make_async_copy(fk_hbm, fkbuf, f_sem.at[0])
    fv_copy = pltpu.make_async_copy(fv_hbm, fvbuf, f_sem.at[1])

    for h in range(heads):
        for g in range(group):
            q_copy(h, g).start()

    barrier = pltpu.get_barrier_semaphore()

    def greet(step, _):
        peer = lax.rem(me + step, devices)
        pl.semaphore_signal(barrier, inc=1, device_id={"ctx": peer}, device_id_type=pl.DeviceIdType.MESH)
        return 0

    lax.fori_loop(1, devices, greet, 0)
    for h in range(heads):
        for g in range(group):
            q_place(h, g).start()
    k_copy(0).start()
    fk_copy.start()
    fv_copy.start()
    v_copy(0).start()
    for h in range(1, heads):
        k_copy(h).start()
        v_copy(h).start()

    row = lax.broadcasted_iota(jnp.int32, (own, rows), 1)
    key = lax.broadcasted_iota(jnp.int32, (own, rows), 0)
    half = tile_pairs * each
    device = lax.div(lax.rem(row, half), each) * 2 + lax.div(row, half)
    relative[...] = device * own + lax.rem(row, own) - key

    for h in range(heads):
        for g in range(group):
            q_copy(h, g).wait()
    pl.semaphore_wait(barrier, devices - 1)

    def gather_copy(h, peer_pair):
        return pltpu.make_async_remote_copy(
            src_ref=qown.at[h], dst_ref=qbuf.at[h, my_tile, core, my_place],
            send_sem=gather_send.at[h], recv_sem=gather_recv.at[h, my_tile],
            device_id={"ctx": peer_pair * 2 + core}, device_id_type=pl.DeviceIdType.MESH,
        )

    def gather(u, _):
        h, step, tile = unit(u)

        def send(j, _):
            gather_copy(h, tile * tile_pairs + lax.rem(my_place + j, tile_pairs)).start()
            return 0

        return lax.fori_loop(jnp.where(step == 0, 1, 0), tile_pairs, send, 0)

    lax.fori_loop(0, units, gather, 0)

    def relay_copy(h, tile):
        mine = qbuf.at[h, tile, core]
        return pltpu.make_async_remote_copy(
            src_ref=mine, dst_ref=mine, send_sem=relay_send.at[h, tile], recv_sem=relay_recv.at[h, tile],
            device_id={"ctx": pair * 2 + 1 - core}, device_id_type=pl.DeviceIdType.MESH,
        )

    def relay(u):
        h, _, tile = unit(u)
        mine = qbuf.at[h, tile, core]
        pltpu.make_async_copy(mine, mine, gather_recv.at[h, tile]).wait()
        relay_copy(h, tile).start()

    def await_queries(u):
        h, step, tile = unit(u)
        relay_copy(h, tile).wait_recv()

        @pl.when((u < early) | ((step == 1) & (h >= early)))
        def _():
            k_copy(h).wait()
            v_copy(h).wait()

    score_slots = (scores_even, scores_odd)

    def score_piece(h, queries, b, j):
        keys = kbuf[h, pl.ds(b * block + j * PIECE_KEYS, PIECE_KEYS), :]
        s = nt_dot(keys, queries)
        score_slots[b % 2][pl.ds(j * PIECE_KEYS, PIECE_KEYS), :] = s
        return fold(s.reshape(PIECE_KEYS // SUBLANES, SUBLANES, rows), jnp.maximum)

    def score_fresh(h, tile, queries):
        s = nt_dot(fkbuf[:, head_columns(h)], queries)
        seen = relative[...] >= (me - tile * 2 * tile_pairs) * own
        s = jnp.where(seen, s, MASKED)
        fresh_scores[...] = s
        return fold(s.reshape(own // SUBLANES, SUBLANES, rows), jnp.maximum)

    def segment(values, scores):
        if values is not None:
            vh, vb = values
            top = jnp.max(block_max[vb % 2], axis=0, keepdims=True)
            if vb > 0:
                before = row_max[0:1]
                top = jnp.maximum(before, top)
                decay = jnp.exp2((before - top) * EXP2_SCALE)
            row_max[0:1] = top
            top8 = jnp.broadcast_to(top, (SUBLANES, rows))
            weights, sums = [], []
        if scores is not None:
            sh, tile, sb = scores
            queries = qbuf[sh, tile].reshape(rows, HEAD_SIZE)
            tops = []
        for j in range(block // PIECE_KEYS):
            if values is not None:
                s = score_slots[vb % 2][pl.ds(j * PIECE_KEYS, PIECE_KEYS), :]
                s = s.reshape(PIECE_KEYS // SUBLANES, SUBLANES, rows)
                p = jnp.exp2((s - top8[None]) * EXP2_SCALE)
                sums.append(fold(p, jnp.add))
                weights.append(p.reshape(PIECE_KEYS, rows).astype(BF16))
            if scores is not None:
                tops.append(score_piece(sh, queries, sb, j))
        if scores is not None:
            if sb == 0:
                tops.append(score_fresh(sh, tile, queries))
            block_max[sb % 2] = functools.reduce(jnp.maximum, tops)
        if values is not None:
            out = tn_dot(vbuf[vh, pl.ds(vb * block, block), :], jnp.concatenate(weights, axis=0))
            if vb == 0:
                s = fresh_scores[...].reshape(own // SUBLANES, SUBLANES, rows)
                p = jnp.exp2((s - top8[None]) * EXP2_SCALE)
                sums.append(fold(p, jnp.add))
                out = out + tn_dot(fvbuf[:, head_columns(vh)], p.reshape(own, rows).astype(BF16))
            total = functools.reduce(jnp.add, sums)
            if vb == 0:
                row_sum[...] = total
                acc[...] = out
            else:
                row_sum[...] = row_sum[...] * decay + total
                acc[...] = acc[...] * decay + out

    def close(u):
        total = jnp.sum(row_sum[...], axis=0, keepdims=True)
        upper = lax.broadcasted_iota(jnp.int32, (SUBLANES, half), 0) < SUM_ROW
        for c in range(2):
            span = slice(c * half, (c + 1) * half)
            obuf[u, c, :HEAD_SIZE] = acc[:, span]
            obuf[u, c, HEAD_SIZE:] = jnp.where(upper, row_max[0:1, span], total[:, span])

    def exchange_copy(u):
        return pltpu.make_async_remote_copy(
            src_ref=obuf.at[u, 1 - core], dst_ref=xbuf.at[u], send_sem=x_send.at[u], recv_sem=x_recv.at[u],
            device_id={"ctx": pair * 2 + 1 - core}, device_id_type=pl.DeviceIdType.MESH,
        )

    def merge(u):
        own_part, other_part = obuf[u, core, HEAD_SIZE:], xbuf[u, HEAD_SIZE:]
        top_a, top_b = own_part[:1], other_part[:1]
        sum_a, sum_b = own_part[SUM_ROW:SUM_ROW + 1], other_part[SUM_ROW:SUM_ROW + 1]
        top = jnp.maximum(top_a, top_b)
        scale_a = jnp.exp2((top_a - top) * EXP2_SCALE)
        scale_b = jnp.exp2((top_b - top) * EXP2_SCALE)
        total = sum_a * scale_a + sum_b * scale_b
        out = obuf[u, core, :HEAD_SIZE] * (scale_a / total) + xbuf[u, :HEAD_SIZE] * (scale_b / total)
        sbuf[u] = out.T.astype(BF16).reshape(tile_pairs, each, HEAD_SIZE)
        mbuf[u, 0:1] = top
        mbuf[u, 1:2] = total

    def out_copy(u, h, tile, place):
        return pltpu.make_async_remote_copy(
            src_ref=sbuf.at[u, place], dst_ref=rbuf.at[h, pair], send_sem=o_send.at[h], recv_sem=o_recv.at[h],
            device_id={"ctx": (tile * tile_pairs + place) * 2 + core}, device_id_type=pl.DeviceIdType.MESH,
        )

    def sums_copy(u, h, tile, place):
        return pltpu.make_async_remote_copy(
            src_ref=mbuf.at[u], dst_ref=rmbuf.at[h, pair], send_sem=m_send.at[h], recv_sem=m_recv.at[h],
            device_id={"ctx": (tile * tile_pairs + place) * 2 + core}, device_id_type=pl.DeviceIdType.MESH,
        )

    def send_out(u):
        h, step, tile = unit(u)

        def send(j, _):
            place = lax.rem(my_place + j, tile_pairs)
            sums_copy(u, h, tile, place).start()
            out_copy(u, h, tile, place).start()
            return 0

        lax.fori_loop(jnp.where(step == 0, 1, 0), tile_pairs, send, 0)

        @pl.when(step == 0)
        def _():
            rbuf[h, pair] = sbuf[u, my_place]
            rmbuf[h, pair] = mbuf[u]

    def incoming(ref, h, sem):
        part = ref.at[h, pl.ds(0, pairs - 1)]
        return pltpu.make_async_copy(part, part, sem.at[h])

    def combine(h):
        incoming(rmbuf, h, m_recv).wait()
        incoming(rbuf, h, o_recv).wait()
        tops, sums = rmbuf[h, :, 0, :], rmbuf[h, :, 1, :]
        weights = jnp.exp2((tops - jnp.max(tops, axis=0, keepdims=True)) * EXP2_SCALE) * sums
        weights = weights / jnp.sum(weights, axis=0, keepdims=True)
        mine = jnp.zeros((pairs, each), F32)
        for place in range(tile_pairs):
            mine = jnp.where(my_place == place, weights[:, place * each:(place + 1) * each], mine)
        diagonal = lax.broadcasted_iota(jnp.int32, (each, each), 0) == lax.broadcasted_iota(
            jnp.int32, (each, each), 1
        )
        result = jnp.zeros((each, HEAD_SIZE), F32)
        for source in range(pairs):
            line = jnp.broadcast_to(mine[source:source + 1, :], (each, each))
            column = jnp.sum(jnp.where(diagonal, line, 0.0), axis=1, keepdims=True)
            result = result + column * rbuf[h, source].astype(F32)
        for g in range(group):
            columns = pl.ds(pl.multiple_of((h * group + g) * HEAD_SIZE, HEAD_SIZE), HEAD_SIZE)
            out_ref[:, columns] = result[g * own:(g + 1) * own].astype(out_ref.dtype)

    def body(u, first=False, second=False):
        h, _, tile = unit(u)
        await_queries(u)
        if not first and not second:
            exchange_copy(u - 2).wait_recv()

        @pl.when(u + 2 < units)
        def _():
            relay(u + 2)

        if first:
            segment(None, (h, tile, 0))
        else:
            segment((unit(u - 1)[0], blocks - 1), (h, tile, 0))
            close(u - 1)
            if not second:
                merge(u - 2)
        for b in range(1, blocks):
            segment((h, b - 1), (h, tile, b))
            if b == 1 and not first:
                exchange_copy(u - 1).start()
                if not second:
                    send_out(u - 2)

    relay(0)
    if units > 1:
        relay(1)
    fk_copy.wait()
    fv_copy.wait()
    body(jnp.int32(0), first=True)
    if units > 1:
        body(jnp.int32(1), second=True)
    lax.fori_loop(2, units, lambda u, _: (body(u), 0)[1], 0)
    last = units - 1
    if units > 1:
        exchange_copy(last - 1).wait_recv()
        merge(last - 1)
    segment((unit(jnp.int32(last))[0], blocks - 1), None)
    close(last)
    exchange_copy(last).start()
    if units > 1:
        send_out(jnp.int32(last - 1))
    lax.fori_loop(0, heads // 2, lambda h, _: (combine(h), 0)[1], 0)
    exchange_copy(last).wait_recv()
    merge(last)
    send_out(jnp.int32(last))
    lax.fori_loop(heads // 2, heads, lambda h, _: (combine(h), 0)[1], 0)

    def drain(h, _):
        incoming(rbuf, h, gather_send).wait()
        incoming(rmbuf, h, m_send).wait()
        incoming(rbuf, h, o_send).wait()
        return 0

    def drain_unit(u, _):
        h, _, tile = unit(u)
        relay_copy(h, tile).wait_send()
        exchange_copy(u).wait_send()
        return 0

    lax.fori_loop(0, heads, drain, 0)
    lax.fori_loop(0, units, drain_unit, 0)


def solution(mesh):
    devices = mesh.shape["ctx"]

    def shards(queries, cache_keys, prefix_values, incoming_keys, incoming_values):
        own = queries.shape[0]
        heads = cache_keys.shape[1] // HEAD_SIZE
        group = queries.shape[1] // cache_keys.shape[1]
        depth = cache_keys.shape[0]
        each = group * own
        pairs = devices // 2
        tile_pairs = min(pairs, TILE_ROWS // (2 * each))
        tiles = pairs // tile_pairs
        rows = 2 * tile_pairs * each
        units = heads * tiles
        block = min(BLOCK_KEYS, depth // 2)
        dma = pltpu.SemaphoreType.DMA
        return pl.pallas_call(
            functools.partial(kernel, devices, heads, group, own, block),
            out_shape=jax.ShapeDtypeStruct(queries.shape, queries.dtype),
            in_specs=[pl.BlockSpec(memory_space=pl.ANY)] * 5,
            out_specs=pl.BlockSpec(memory_space=pltpu.VMEM),
            scratch_shapes=[
                pltpu.VMEM((heads, each, HEAD_SIZE), BF16),
                pltpu.VMEM((heads, tiles, 2, tile_pairs, each, HEAD_SIZE), BF16),
                pltpu.VMEM((heads, depth, HEAD_SIZE), BF16),
                pltpu.VMEM((heads, depth, HEAD_SIZE), BF16),
                pltpu.VMEM((own, heads * HEAD_SIZE), BF16),
                pltpu.VMEM((own, heads * HEAD_SIZE), BF16),
                pltpu.VMEM((block, rows), F32),
                pltpu.VMEM((block, rows), F32),
                pltpu.VMEM((own, rows), F32),
                pltpu.VMEM((own, rows), jnp.int32),
                pltpu.VMEM((2, SUBLANES, rows), F32),
                pltpu.VMEM((SUBLANES, rows), F32),
                pltpu.VMEM((SUBLANES, rows), F32),
                pltpu.VMEM((HEAD_SIZE, rows), F32),
                pltpu.VMEM((units, 2, HEAD_SIZE + SUBLANES, rows // 2), F32),
                pltpu.VMEM((units, HEAD_SIZE + SUBLANES, rows // 2), F32),
                pltpu.VMEM((units, tile_pairs, each, HEAD_SIZE), BF16),
                pltpu.VMEM((units, 2, rows // 2), F32),
                pltpu.VMEM((heads, pairs, each, HEAD_SIZE), BF16),
                pltpu.VMEM((heads, pairs, 2, rows // 2), F32),
                dma((heads, group)), dma((heads,)), dma((heads,)), dma((2,)),
                dma((heads,)), dma((heads, tiles)), dma((heads, tiles)), dma((heads, tiles)),
                dma((units,)), dma((units,)), dma((heads,)), dma((heads,)), dma((heads,)), dma((heads,)),
            ],
            compiler_params=pltpu.CompilerParams(
                collective_id=0, has_side_effects=True, vmem_limit_bytes=60 * 1024 * 1024
            ),
        )(queries, cache_keys, prefix_values, incoming_keys, incoming_values)

    spec = P("ctx", "head")
    return jax.shard_map(
        shards, mesh=mesh, in_specs=(spec,) * 5, out_specs=spec, check_vma=False
    )
```

```python
import functools
import math

import jax
import jax.numpy as jnp
from jax import lax
from jax.experimental import pallas as pl
from jax.experimental.pallas import tpu as pltpu
from jax.sharding import PartitionSpec as P

HEAD_SIZE = 128
LANES = 128
SUBLANES = 8
SUM_ROW = 4
TILE_ROWS = 256
BLOCK_KEYS = 1024
PIECE_KEYS = 256
EXP2_SCALE = 168.0 ** (-0.5) * math.log2(math.e)
MASKED = -1e30
BF16, F32 = jnp.bfloat16, jnp.float32


def nt_dot(a, b):
    return lax.dot_general(a, b, (((1,), (1,)), ((), ())), preferred_element_type=F32)


def tn_dot(a, b):
    return lax.dot_general(a, b, (((0,), (0,)), ((), ())), preferred_element_type=F32)


def fold(x, op):
    parts = [x[i] for i in range(x.shape[0])]
    while len(parts) > 1:
        parts = [op(*parts[i:i + 2]) if i + 1 < len(parts) else parts[i] for i in range(0, len(parts), 2)]
    return parts[0]


def kernel(
    devices, heads, group, own, block,
    q_hbm, k_hbm, v_hbm, fk_hbm, fv_hbm, out_ref,
    qbuf, kbuf, vbuf, fkbuf, fvbuf, scores_even, scores_odd, fresh_scores, relative,
    block_max, row_max, row_sum, acc, obuf, xbuf, sbuf, smbuf, nbuf, nmbuf, hbuf, hmbuf, fbuf, fmbuf,
    k_sem, v_sem, f_sem, ready, block_recv, gather_recv, relay_recv, x_recv, n_recv, nm_recv, far_recv, farm_recv,
    far_query_send, gather_send, relay_send, x_send, n_send, nm_send, far_send, farm_send,
):
    tiles, tile_pairs = qbuf.shape[1], qbuf.shape[3]
    each = group * own
    half = tile_pairs * each
    rows = 2 * half
    tile_devices = 2 * tile_pairs
    blocks = kbuf.shape[1] // block
    units = heads * tiles
    early = heads // 2 if tiles > 1 else heads
    late = early + heads * (tiles - 1)
    me = lax.axis_index("ctx")
    core, pair = lax.rem(me, 2), lax.div(me, 2)
    my_tile, my_place = lax.div(pair, tile_pairs), lax.rem(pair, tile_pairs)

    def is_far(u):
        return (u >= early) & (u < late)

    def unit(u):
        far = jnp.maximum(u - early, 0)
        near = jnp.where(u < early, u, u - heads * (tiles - 1))
        h = jnp.where(is_far(u), lax.rem(far, heads), near)
        step = jnp.where(is_far(u), 1 + lax.div(far, heads), 0)
        return h, step, lax.rem(my_tile + step, tiles)

    def near_unit(h):
        return jnp.where(h < early, h, h + heads * (tiles - 1))

    def neighbour(j):
        return {"ctx": (my_tile * tile_pairs + lax.rem(my_place + j, tile_pairs)) * 2 + core}

    sibling = {"ctx": pair * 2 + 1 - core}

    def partner(tile):
        return {"ctx": (tile * tile_pairs + my_place) * 2 + core}

    def remote(src, dst, send_sem, recv_sem, device):
        return pltpu.make_async_remote_copy(
            src_ref=src, dst_ref=dst, send_sem=send_sem, recv_sem=recv_sem,
            device_id=device, device_id_type=pl.DeviceIdType.MESH,
        )

    def await_bytes(ref, sem):
        pltpu.make_async_copy(ref, ref, sem).wait()

    def head_columns(h):
        return pl.ds(pl.multiple_of(h * HEAD_SIZE, HEAD_SIZE), HEAD_SIZE)

    def k_copy(h):
        return pltpu.make_async_copy(k_hbm.at[:, head_columns(h)], kbuf.at[h], k_sem.at[h])

    def v_copy(h):
        return pltpu.make_async_copy(v_hbm.at[:, head_columns(h)], vbuf.at[h], v_sem.at[h])

    fk_copy = pltpu.make_async_copy(fk_hbm, fkbuf, f_sem.at[0])
    fv_copy = pltpu.make_async_copy(fv_hbm, fvbuf, f_sem.at[1])

    barrier = pltpu.get_barrier_semaphore()

    def signal(sem, device):
        pl.semaphore_signal(sem, inc=1, device_id=device, device_id_type=pl.DeviceIdType.MESH)

    for j in range(1, tile_devices):
        signal(barrier, {"ctx": my_tile * tile_devices + lax.rem(lax.rem(me, tile_devices) + j, tile_devices)})
    lax.fori_loop(my_tile + 1, tiles, lambda t, _: (signal(barrier, partner(t)), 0)[1], 0)

    for h in range(heads):
        for g in range(group):
            columns = pl.ds((h * group + g) * HEAD_SIZE, HEAD_SIZE)
            pltpu.make_async_copy(
                q_hbm.at[:, columns], qbuf.at[h, my_tile, core, my_place, pl.ds(g * own, own)],
                block_recv.at[h, my_tile],
            ).start()
    k_copy(0).start()
    fk_copy.start()
    fv_copy.start()
    v_copy(0).start()

    row = lax.broadcasted_iota(jnp.int32, (own, rows), 1)
    key = lax.broadcasted_iota(jnp.int32, (own, rows), 0)
    device = lax.div(lax.rem(row, half), each) * 2 + lax.div(row, half)
    relative[...] = device * own + lax.rem(row, own) - key

    def await_block(h, tile):
        await_bytes(qbuf.at[h, tile, core, my_place], block_recv.at[h, tile])

    def forward(h, tile):
        mine = qbuf.at[h, tile, core, my_place]
        for j in range(1, tile_pairs):
            remote(mine, mine, gather_send.at[0], gather_recv.at[h, tile], neighbour(j)).start()

    def relay_copy(h, tile):
        mine = qbuf.at[h, tile, core]
        return remote(mine, mine, relay_send.at[0], relay_recv.at[h, tile], sibling)

    def relay(h, tile):
        await_bytes(qbuf.at[h, tile, core, pl.ds(0, tile_pairs - 1)], gather_recv.at[h, tile])
        relay_copy(h, tile).start()

    def await_queries(u):
        h, step, tile = unit(u)
        relay_copy(h, tile).wait_recv()

        @pl.when((u < early) | ((step == 1) & (h >= early)))
        def _():
            k_copy(h).wait()
            v_copy(h).wait()

    score_slots = (scores_even, scores_odd)

    def score_piece(h, queries, b, j):
        keys = kbuf[h, pl.ds(b * block + j * PIECE_KEYS, PIECE_KEYS), :]
        s = nt_dot(keys, queries)
        score_slots[b % 2][pl.ds(j * PIECE_KEYS, PIECE_KEYS), :] = s
        return fold(s.reshape(PIECE_KEYS // SUBLANES, SUBLANES, rows), jnp.maximum)

    def score_fresh(h, tile, queries):
        s = nt_dot(fkbuf[:, head_columns(h)], queries)
        seen = relative[...] >= (me - tile * tile_devices) * own
        s = jnp.where(seen, s, MASKED)
        fresh_scores[...] = s
        return fold(s.reshape(own // SUBLANES, SUBLANES, rows), jnp.maximum)

    def segment(values, scores, finish=None):
        if values is not None:
            vh, vb = values
            top = jnp.max(block_max[vb % 2], axis=0, keepdims=True)
            if vb > 0:
                before = row_max[0:1]
                top = jnp.maximum(before, top)
                decay = jnp.exp2((before - top) * EXP2_SCALE)
            row_max[0:1] = top
            top8 = jnp.broadcast_to(top, (SUBLANES, rows))
            weights, sums = [], []
        if scores is not None:
            sh, tile, sb = scores
            queries = qbuf[sh, tile].reshape(rows, HEAD_SIZE)
            tops = []
        for j in range(block // PIECE_KEYS):
            if values is not None:
                s = score_slots[vb % 2][pl.ds(j * PIECE_KEYS, PIECE_KEYS), :]
                s = s.reshape(PIECE_KEYS // SUBLANES, SUBLANES, rows)
                p = jnp.exp2((s - top8[None]) * EXP2_SCALE)
                sums.append(fold(p, jnp.add))
                weights.append(p.reshape(PIECE_KEYS, rows).astype(BF16))
            if scores is not None:
                tops.append(score_piece(sh, queries, sb, j))
        if scores is not None:
            if sb == 0:
                tops.append(score_fresh(sh, tile, queries))
            block_max[sb % 2] = functools.reduce(jnp.maximum, tops)
        if values is not None:
            out = tn_dot(vbuf[vh, pl.ds(vb * block, block), :], jnp.concatenate(weights, axis=0))
            if vb == 0:
                s = fresh_scores[...].reshape(own // SUBLANES, SUBLANES, rows)
                p = jnp.exp2((s - top8[None]) * EXP2_SCALE)
                sums.append(fold(p, jnp.add))
                out = out + tn_dot(fvbuf[:, head_columns(vh)], p.reshape(own, rows).astype(BF16))
            total = functools.reduce(jnp.add, sums)
            if vb > 0:
                total = row_sum[...] * decay + total
                out = acc[...] * decay + out
            if finish is None:
                row_sum[...] = total
                acc[...] = out
            else:
                total = jnp.sum(total, axis=0, keepdims=True)
                upper = lax.broadcasted_iota(jnp.int32, (SUBLANES, half), 0) < SUM_ROW
                for c in range(2):
                    span = slice(c * half, (c + 1) * half)
                    obuf[finish, c, :HEAD_SIZE] = out[:, span]
                    obuf[finish, c, HEAD_SIZE:] = jnp.where(upper, top[:, span], total[:, span])

    def exchange_copy(u):
        return remote(obuf.at[u, 1 - core], xbuf.at[u], x_send.at[0], x_recv.at[u], sibling)

    def merge_cores(u):
        own_part, other_part = obuf[u, core, HEAD_SIZE:], xbuf[u, HEAD_SIZE:]
        top_a, top_b = own_part[:1], other_part[:1]
        sum_a, sum_b = own_part[SUM_ROW:SUM_ROW + 1], other_part[SUM_ROW:SUM_ROW + 1]
        top = jnp.maximum(top_a, top_b)
        scale_a = jnp.exp2((top_a - top) * EXP2_SCALE)
        scale_b = jnp.exp2((top_b - top) * EXP2_SCALE)
        total = sum_a * scale_a + sum_b * scale_b
        out = obuf[u, core, :HEAD_SIZE] * (scale_a / total) + xbuf[u, :HEAD_SIZE] * (scale_b / total)
        sbuf[u] = out.T.astype(BF16).reshape(tile_pairs, each, HEAD_SIZE)
        smbuf[u, 0:1] = top
        smbuf[u, 1:2] = total
        nbuf[u, my_place] = sbuf[u, my_place]
        nmbuf[u, my_place] = smbuf[u]

    def scatter(u):
        for j in range(1, tile_pairs):
            place = lax.rem(my_place + j, tile_pairs)
            remote(smbuf.at[u], nmbuf.at[u, my_place], nm_send.at[0], nm_recv.at[u], neighbour(j)).start()
            remote(sbuf.at[u, place], nbuf.at[u, my_place], n_send.at[0], n_recv.at[u], neighbour(j)).start()

    def await_scattered(u):
        await_bytes(nmbuf.at[u, pl.ds(0, tile_pairs - 1)], nm_recv.at[u])
        await_bytes(nbuf.at[u, pl.ds(0, tile_pairs - 1)], n_recv.at[u])

    def mix(tops, sums, parts):
        top = jnp.max(tops, axis=0, keepdims=True)
        weights = jnp.exp2((tops - top) * EXP2_SCALE) * sums
        total = jnp.sum(weights, axis=0, keepdims=True)
        weights = weights / total
        mine = jnp.zeros((len(parts), each), F32)
        for place in range(tile_pairs):
            mine = jnp.where(my_place == place, weights[:, place * each:(place + 1) * each], mine)
        diagonal = lax.broadcasted_iota(jnp.int32, (each, each), 0) == lax.broadcasted_iota(
            jnp.int32, (each, each), 1
        )
        result = jnp.zeros((each, HEAD_SIZE), F32)
        for source, part in enumerate(parts):
            line = jnp.broadcast_to(mine[source:source + 1, :], (each, each))
            column = jnp.sum(jnp.where(diagonal, line, 0.0), axis=1, keepdims=True)
            result = result + column * part.astype(F32)
        return result, top, total

    def merge_tile(u):
        h, _, tile = unit(u)
        await_scattered(u)
        result, top, total = mix(
            nmbuf[u, :, 0, :], nmbuf[u, :, 1, :], [nbuf[u, place] for place in range(tile_pairs)]
        )
        hbuf[h, tile] = result.astype(BF16)
        hmbuf[h, tile, 0:1] = top
        hmbuf[h, tile, 1:2] = total
        remote(
            hmbuf.at[h, tile], fmbuf.at[h, my_tile], farm_send.at[0], farm_recv.at[h], partner(tile)
        ).start()
        remote(hbuf.at[h, tile], fbuf.at[h, my_tile], far_send.at[0], far_recv.at[h], partner(tile)).start()

    def combine(h):
        u = near_unit(h)
        await_scattered(u)
        tops, sums = [nmbuf[u, :, 0, :]], [nmbuf[u, :, 1, :]]
        parts = [nbuf[u, place] for place in range(tile_pairs)]
        if tiles > 1:
            await_bytes(fmbuf.at[h, pl.ds(0, tiles - 1)], farm_recv.at[h])
            await_bytes(fbuf.at[h, pl.ds(0, tiles - 1)], far_recv.at[h])
        for step in range(1, tiles):
            tile = lax.rem(my_tile + step, tiles)
            tops.append(fmbuf[h, tile, 0:1])
            sums.append(fmbuf[h, tile, 1:2])
            parts.append(fbuf[h, tile])
        result, _, _ = mix(jnp.concatenate(tops, axis=0), jnp.concatenate(sums, axis=0), parts)
        for g in range(group):
            columns = pl.ds(pl.multiple_of((h * group + g) * HEAD_SIZE, HEAD_SIZE), HEAD_SIZE)
            out_ref[:, columns] = result[g * own:(g + 1) * own].astype(out_ref.dtype)

    def body(u, peeled=3):
        h, _, tile = unit(u)
        await_queries(u)

        @pl.when(u + 2 < heads)
        def _():
            k_copy(u + 2).start()
            v_copy(u + 2).start()

        if peeled > 2:
            exchange_copy(u - 3).wait_recv()
        if peeled > 0:
            for v in (2 * u + 2, 2 * u + 3):

                @pl.when(is_far(v))
                def _(v=v):
                    far_head, _, far_tile = unit(v)
                    await_block(far_head, far_tile)
                    forward(far_head, far_tile)

        @pl.when(u + 1 < units)
        def _():
            next_head, _, next_tile = unit(u + 1)
            relay(next_head, next_tile)

        if peeled > 2:

            @pl.when(is_far(u - 6))
            def _():
                merge_tile(u - 6)

        if peeled == 0:
            segment(None, (h, tile, 0))
        else:
            segment((unit(u - 1)[0], blocks - 1), (h, tile, 0), finish=u - 1)
        for b in range(1, blocks):
            segment((h, b - 1), (h, tile, b))
            if b == 1 and peeled > 2:
                merge_cores(u - 3)
        if peeled > 0:
            exchange_copy(u - 1).start()
        if peeled > 2:
            scatter(u - 3)

    pl.semaphore_wait(barrier, tile_devices - 1 + my_tile)
    for h in range(heads):
        await_block(h, my_tile)
    for h in range(early):
        forward(h, my_tile)
    lax.fori_loop(0, my_tile, lambda t, _: (signal(ready, partner(t)), 0)[1], 0)

    @pl.when(my_tile < tiles - 1)
    def _():
        pl.semaphore_wait(ready, tiles - 1 - my_tile)

    for step in range(1, tiles):
        tile = lax.rem(my_tile + step, tiles)
        for h in range(heads):
            mine = qbuf.at[h, my_tile, core, my_place]
            remote(mine, mine, far_query_send.at[0], block_recv.at[h, my_tile], partner(tile)).start()
    for h in range(early, heads):
        forward(h, my_tile)
    for u in range(early, min(4, late)):
        far_head, _, far_tile = unit(jnp.int32(u))
        await_block(far_head, far_tile)
        forward(far_head, far_tile)
    if heads > 1:
        k_copy(1).start()
        v_copy(1).start()
    first_head, _, first_tile = unit(jnp.int32(0))
    relay(first_head, first_tile)
    fk_copy.wait()
    fv_copy.wait()
    for u in range(min(3, units)):
        body(jnp.int32(u), u)
    lax.fori_loop(3, units, lambda u, _: (body(u), 0)[1], 0)

    def merge_and_scatter(u):
        exchange_copy(u).wait_recv()
        merge_cores(u)
        scatter(u)

    last = units - 1
    segment((unit(jnp.int32(last))[0], blocks - 1), None, finish=last)
    exchange_copy(last).start()
    for u in range(max(0, units - 3), last):
        merge_and_scatter(u)
    for u in range(max(early, units - 6), min(late, last)):
        merge_tile(jnp.int32(u))
    if late == units:
        merge_and_scatter(last)
        if tiles > 1:
            merge_tile(jnp.int32(last))
        lax.fori_loop(0, heads, lambda h, _: (combine(h), 0)[1], 0)
    else:
        lax.fori_loop(0, heads - 2, lambda h, _: (combine(h), 0)[1], 0)
        merge_and_scatter(last)
        lax.fori_loop(max(0, heads - 2), heads, lambda h, _: (combine(h), 0)[1], 0)

    await_bytes(sbuf.at[:, pl.ds(0, tile_pairs - 1)], gather_send.at[0])
    await_bytes(sbuf, relay_send.at[0])
    await_bytes(xbuf, x_send.at[0])
    await_bytes(nmbuf.at[:, pl.ds(0, tile_pairs - 1)], nm_send.at[0])
    await_bytes(nbuf.at[:, pl.ds(0, tile_pairs - 1)], n_send.at[0])
    if tiles > 1:
        await_bytes(fbuf.at[:, pl.ds(0, tiles - 1)], far_query_send.at[0])
        await_bytes(fmbuf.at[:, pl.ds(0, tiles - 1)], farm_send.at[0])
        await_bytes(fbuf.at[:, pl.ds(0, tiles - 1)], far_send.at[0])


def solution(mesh):
    devices = mesh.shape["ctx"]

    def shards(queries, cache_keys, prefix_values, incoming_keys, incoming_values):
        own = queries.shape[0]
        heads = cache_keys.shape[1] // HEAD_SIZE
        group = queries.shape[1] // cache_keys.shape[1]
        depth = cache_keys.shape[0]
        each = group * own
        pairs = devices // 2
        tile_pairs = min(pairs, TILE_ROWS // (2 * each))
        tiles = pairs // tile_pairs
        rows = 2 * tile_pairs * each
        units = heads * tiles
        block = min(BLOCK_KEYS, depth // 2)
        dma = pltpu.SemaphoreType.DMA
        return pl.pallas_call(
            functools.partial(kernel, devices, heads, group, own, block),
            out_shape=jax.ShapeDtypeStruct(queries.shape, queries.dtype),
            in_specs=[pl.BlockSpec(memory_space=pl.ANY)] * 5,
            out_specs=pl.BlockSpec(memory_space=pltpu.VMEM),
            scratch_shapes=[
                pltpu.VMEM((heads, tiles, 2, tile_pairs, each, HEAD_SIZE), BF16),
                pltpu.VMEM((heads, depth, HEAD_SIZE), BF16),
                pltpu.VMEM((heads, depth, HEAD_SIZE), BF16),
                pltpu.VMEM((own, heads * HEAD_SIZE), BF16),
                pltpu.VMEM((own, heads * HEAD_SIZE), BF16),
                pltpu.VMEM((block, rows), F32),
                pltpu.VMEM((block, rows), F32),
                pltpu.VMEM((own, rows), F32),
                pltpu.VMEM((own, rows), jnp.int32),
                pltpu.VMEM((2, SUBLANES, rows), F32),
                pltpu.VMEM((SUBLANES, rows), F32),
                pltpu.VMEM((SUBLANES, rows), F32),
                pltpu.VMEM((HEAD_SIZE, rows), F32),
                pltpu.VMEM((units, 2, HEAD_SIZE + SUBLANES, rows // 2), F32),
                pltpu.VMEM((units, HEAD_SIZE + SUBLANES, rows // 2), F32),
                pltpu.VMEM((units, tile_pairs, each, HEAD_SIZE), BF16),
                pltpu.VMEM((units, 2, rows // 2), F32),
                pltpu.VMEM((units, tile_pairs, each, HEAD_SIZE), BF16),
                pltpu.VMEM((units, tile_pairs, 2, rows // 2), F32),
                pltpu.VMEM((heads, tiles, each, HEAD_SIZE), BF16),
                pltpu.VMEM((heads, tiles, 2, rows // 2), F32),
                pltpu.VMEM((heads, tiles, each, HEAD_SIZE), BF16),
                pltpu.VMEM((heads, tiles, 2, rows // 2), F32),
                dma((heads,)), dma((heads,)), dma((2,)), pltpu.SemaphoreType.REGULAR,
                dma((heads, tiles)), dma((heads, tiles)), dma((heads, tiles)),
                dma((units,)), dma((units,)), dma((units,)), dma((heads,)), dma((heads,)),
                *[dma((1,))] * 8,
            ],
            compiler_params=pltpu.CompilerParams(
                collective_id=0, has_side_effects=True, vmem_limit_bytes=60 * 1024 * 1024
            ),
        )(queries, cache_keys, prefix_values, incoming_keys, incoming_values)

    spec = P("ctx", "head")
    return jax.shard_map(
        shards, mesh=mesh, in_specs=(spec,) * 5, out_specs=spec, check_vma=False
    )
```

```python
import functools
import math

import jax
import jax.numpy as jnp
from jax import lax
from jax.experimental import pallas as pl
from jax.experimental.pallas import tpu as pltpu
from jax.sharding import PartitionSpec as P

HEAD_SIZE = 128
LANES = 128
SUBLANES = 8
SUM_ROW = 4
STAT_ROWS = 16
SUM_ROWS = 16
LAG = 3
TILE_ROWS = 256
BLOCK_KEYS = 1024
PIECE_KEYS = 256
EXP2_SCALE = 168.0 ** (-0.5) * math.log2(math.e)
MASKED = -1e30
BF16, F32 = jnp.bfloat16, jnp.float32


def nt_dot(a, b):
    return lax.dot_general(a, b, (((1,), (1,)), ((), ())), preferred_element_type=F32)


def weigh(values, weights):
    ones = jnp.ones((SUM_ROWS, values.shape[0]), BF16)
    return jnp.dot(jnp.concatenate([values.T, ones], axis=0), weights, preferred_element_type=F32)


def stats_rows(top, total):
    rows, parts = lax.broadcasted_iota(jnp.int32, (STAT_ROWS, top.shape[1]), 0), []
    for value in (top, total):
        high = value.astype(BF16).astype(F32)
        middle = (value - high).astype(BF16).astype(F32)
        parts += [high, middle, value - high - middle]
    out = jnp.zeros(rows.shape, F32)
    for i, part in enumerate(parts):
        out = jnp.where(rows == i, part, out)
    return out.astype(BF16)


def read_stats(rows):
    x = rows.astype(F32)
    return x[0:1] + x[1:2] + x[2:3], x[3:4] + x[4:5] + x[5:6]


def fold(x, op):
    parts = [x[i] for i in range(x.shape[0])]
    while len(parts) > 1:
        parts = [op(*parts[i:i + 2]) if i + 1 < len(parts) else parts[i] for i in range(0, len(parts), 2)]
    return parts[0]


def kernel(
    devices, heads, group, own, block,
    q_hbm, k_hbm, v_hbm, fk_hbm, fv_hbm, out_ref,
    qbuf, kbuf, vbuf, fkbuf, fvbuf, scores_even, scores_odd, fresh_scores, relative,
    block_max, row_max, acc, obuf, xbuf, sbuf, nbuf, hbuf, fbuf, dbuf, lbuf,
    k_sem, v_sem, f_sem, ready, block_recv, gather_recv, relay_recv, x_recv, n_recv, far_recv, d_recv,
    far_query_send, gather_send, relay_send, x_send, n_send, far_send, d_send,
):
    tiles, tile_pairs = qbuf.shape[1], qbuf.shape[3]
    each = group * own
    half = tile_pairs * each
    rows = 2 * half
    tile_devices = 2 * tile_pairs
    blocks = kbuf.shape[1] // block
    units = heads * tiles
    early = heads // 2 if tiles > 1 else heads
    late = early + heads * (tiles - 1)
    direct = min(2, heads - early if tiles > 1 else heads)
    merged = units - direct
    me = lax.axis_index("ctx")
    core, pair = lax.rem(me, 2), lax.div(me, 2)
    my_tile, my_place = lax.div(pair, tile_pairs), lax.rem(pair, tile_pairs)

    def is_far(u):
        return (u >= early) & (u < late)

    def unit(u):
        far = jnp.maximum(u - early, 0)
        near = jnp.where(u < early, u, u - heads * (tiles - 1))
        h = jnp.where(is_far(u), lax.rem(far, heads), near)
        step = jnp.where(is_far(u), 1 + lax.div(far, heads), 0)
        return h, step, lax.rem(my_tile + step, tiles)

    def near_unit(h):
        return jnp.where(h < early, h, h + heads * (tiles - 1))

    def neighbour(j, other=0):
        there = core if other == 0 else 1 - core
        return {"ctx": (my_tile * tile_pairs + lax.rem(my_place + j, tile_pairs)) * 2 + there}

    others = [(j, other) for j in range(tile_pairs - 1, -1, -1) for other in range(2) if j + other > 0]

    sibling = {"ctx": pair * 2 + 1 - core}

    def partner(tile):
        return {"ctx": (tile * tile_pairs + my_place) * 2 + core}

    def remote(src, dst, send_sem, recv_sem, device):
        return pltpu.make_async_remote_copy(
            src_ref=src, dst_ref=dst, send_sem=send_sem, recv_sem=recv_sem,
            device_id=device, device_id_type=pl.DeviceIdType.MESH,
        )

    def await_bytes(ref, sem):
        pltpu.make_async_copy(ref, ref, sem).wait()

    def head_columns(h):
        return pl.ds(pl.multiple_of(h * HEAD_SIZE, HEAD_SIZE), HEAD_SIZE)

    def k_copy(h):
        return pltpu.make_async_copy(k_hbm.at[:, head_columns(h)], kbuf.at[h], k_sem.at[h])

    def v_copy(h):
        return pltpu.make_async_copy(v_hbm.at[:, head_columns(h)], vbuf.at[h], v_sem.at[h])

    fk_copy = pltpu.make_async_copy(fk_hbm, fkbuf, f_sem.at[0])
    fv_copy = pltpu.make_async_copy(fv_hbm, fvbuf, f_sem.at[1])

    barrier = pltpu.get_barrier_semaphore()

    def signal(sem, device):
        pl.semaphore_signal(sem, inc=1, device_id=device, device_id_type=pl.DeviceIdType.MESH)

    for j in range(1, tile_devices):
        signal(barrier, {"ctx": my_tile * tile_devices + lax.rem(lax.rem(me, tile_devices) + j, tile_devices)})
    lax.fori_loop(my_tile + 1, tiles, lambda t, _: (signal(barrier, partner(t)), 0)[1], 0)

    for h in range(heads):
        for g in range(group):
            columns = pl.ds((h * group + g) * HEAD_SIZE, HEAD_SIZE)
            pltpu.make_async_copy(
                q_hbm.at[:, columns], qbuf.at[h, my_tile, core, my_place, pl.ds(g * own, own)],
                block_recv.at[h, my_tile],
            ).start()
    k_copy(0).start()
    fk_copy.start()
    fv_copy.start()
    v_copy(0).start()

    row = lax.broadcasted_iota(jnp.int32, (own, rows), 1)
    key = lax.broadcasted_iota(jnp.int32, (own, rows), 0)
    device = lax.div(lax.rem(row, half), each) * 2 + lax.div(row, half)
    relative[...] = device * own + lax.rem(row, own) - key

    def await_block(h, tile):
        await_bytes(qbuf.at[h, tile, core, my_place], block_recv.at[h, tile])

    def forward(h, tile):
        mine = qbuf.at[h, tile, core, my_place]
        for j in range(1, tile_pairs):
            remote(mine, mine, gather_send.at[0], gather_recv.at[h, tile], neighbour(j)).start()

    def forward_to_all(h):
        mine = qbuf.at[h, my_tile, core, my_place]
        for j, other in others:
            remote(mine, mine, gather_send.at[0], gather_recv.at[h, my_tile], neighbour(j, other)).start()

    def await_all(h):
        await_bytes(sbuf.at[pl.ds(0, len(others)), 0, pl.ds(0, each)], gather_recv.at[h, my_tile])

    def relay_copy(h, tile):
        mine = qbuf.at[h, tile, core]
        return remote(mine, mine, relay_send.at[0], relay_recv.at[h, tile], sibling)

    def relay(h, tile):
        await_bytes(qbuf.at[h, tile, core, pl.ds(0, tile_pairs - 1)], gather_recv.at[h, tile])
        relay_copy(h, tile).start()

    def await_queries(u, peeled):
        h, step, tile = unit(u)
        if peeled == 0 and early > 0:
            await_all(0)
        else:
            relay_copy(h, tile).wait_recv()

        @pl.when((u < early) | ((step == 1) & (h >= early)))
        def _():
            k_copy(h).wait()
            v_copy(h).wait()

    score_slots = (scores_even, scores_odd)

    def score_piece(h, queries, b, j):
        keys = kbuf[h, pl.ds(b * block + j * PIECE_KEYS, PIECE_KEYS), :]
        s = nt_dot(keys, queries)
        score_slots[b % 2][pl.ds(j * PIECE_KEYS, PIECE_KEYS), :] = s
        return fold(s.reshape(PIECE_KEYS // SUBLANES, SUBLANES, rows), jnp.maximum)

    def score_fresh(h, tile, queries):
        s = nt_dot(fkbuf[:, head_columns(h)], queries)
        seen = relative[...] >= (me - tile * tile_devices) * own
        s = jnp.where(seen, s, MASKED)
        fresh_scores[...] = s
        return fold(s.reshape(own // SUBLANES, SUBLANES, rows), jnp.maximum)

    def segment(values, scores, finish=None):
        if values is not None:
            vh, vb = values
            top = jnp.max(block_max[vb % 2], axis=0, keepdims=True)
            if vb > 0:
                before = row_max[0:1]
                top = jnp.maximum(before, top)
                decay = jnp.exp2((before - top) * EXP2_SCALE)
            row_max[0:1] = top
            top8 = jnp.broadcast_to(top, (SUBLANES, rows))
            weights = []
        if scores is not None:
            sh, tile, sb = scores
            queries = qbuf[sh, tile].reshape(rows, HEAD_SIZE)
            tops = []
        for j in range(block // PIECE_KEYS):
            if values is not None:
                s = score_slots[vb % 2][pl.ds(j * PIECE_KEYS, PIECE_KEYS), :]
                s = s.reshape(PIECE_KEYS // SUBLANES, SUBLANES, rows)
                p = jnp.exp2((s - top8[None]) * EXP2_SCALE)
                weights.append(p.reshape(PIECE_KEYS, rows).astype(BF16))
            if scores is not None:
                tops.append(score_piece(sh, queries, sb, j))
        if scores is not None:
            if sb == 0:
                tops.append(score_fresh(sh, tile, queries))
            block_max[sb % 2] = functools.reduce(jnp.maximum, tops)
        if values is not None:
            out = weigh(vbuf[vh, pl.ds(vb * block, block), :], jnp.concatenate(weights, axis=0))
            if vb == 0:
                s = fresh_scores[...].reshape(own // SUBLANES, SUBLANES, rows)
                p = jnp.exp2((s - top8[None]) * EXP2_SCALE)
                out = out + weigh(fvbuf[:, head_columns(vh)], p.reshape(own, rows).astype(BF16))
            if vb > 0:
                out = acc[...] * decay + out
            if finish is None:
                acc[...] = out
            else:
                total = out[HEAD_SIZE:HEAD_SIZE + 1]
                out = out[:HEAD_SIZE]
                upper = lax.broadcasted_iota(jnp.int32, (SUBLANES, half), 0) < SUM_ROW
                for c in range(2):
                    span = slice(c * half, (c + 1) * half)
                    obuf[finish, c, :HEAD_SIZE] = out[:, span]
                    obuf[finish, c, HEAD_SIZE:] = jnp.where(upper, top[:, span], total[:, span])

    def exchange_copy(u):
        return remote(obuf.at[u, 1 - core], xbuf.at[u], x_send.at[0], x_recv.at[u], sibling)

    def merge_cores(u):
        own_part, other_part = obuf[u, core, HEAD_SIZE:], xbuf[u, HEAD_SIZE:]
        top_a, top_b = own_part[:1], other_part[:1]
        sum_a, sum_b = own_part[SUM_ROW:SUM_ROW + 1], other_part[SUM_ROW:SUM_ROW + 1]
        top = jnp.maximum(top_a, top_b)
        scale_a = jnp.exp2((top_a - top) * EXP2_SCALE)
        scale_b = jnp.exp2((top_b - top) * EXP2_SCALE)
        total = sum_a * scale_a + sum_b * scale_b
        out = obuf[u, core, :HEAD_SIZE] * (scale_a / total) + xbuf[u, :HEAD_SIZE] * (scale_b / total)
        sbuf[u, :, :each] = out.T.astype(BF16).reshape(tile_pairs, each, HEAD_SIZE)
        stats = stats_rows(top, total)
        for place in range(tile_pairs):
            sbuf[u, place, each:] = stats
        nbuf[u, my_place] = sbuf[u, my_place]

    def scatter(u):
        for j in range(1, tile_pairs):
            place = lax.rem(my_place + j, tile_pairs)
            remote(sbuf.at[u, place], nbuf.at[u, my_place], n_send.at[0], n_recv.at[u], neighbour(j)).start()

    def await_scattered(u):
        await_bytes(nbuf.at[u, pl.ds(0, tile_pairs - 1)], n_recv.at[u])

    def mix(parts):
        tops, sums = zip(*[read_stats(part[each:]) for part in parts], strict=True)
        tops, sums = jnp.concatenate(tops, axis=0), jnp.concatenate(sums, axis=0)
        top = jnp.max(tops, axis=0, keepdims=True)
        weights = jnp.exp2((tops - top) * EXP2_SCALE) * sums
        total = jnp.sum(weights, axis=0, keepdims=True)
        weights = weights / total
        mine = jnp.zeros((len(parts), each), F32)
        for place in range(tile_pairs):
            mine = jnp.where(my_place == place, weights[:, place * each:(place + 1) * each], mine)
        diagonal = lax.broadcasted_iota(jnp.int32, (each, each), 0) == lax.broadcasted_iota(
            jnp.int32, (each, each), 1
        )
        result = jnp.zeros((each, HEAD_SIZE), F32)
        for source, part in enumerate(parts):
            line = jnp.broadcast_to(mine[source:source + 1, :], (each, each))
            column = jnp.sum(jnp.where(diagonal, line, 0.0), axis=1, keepdims=True)
            result = result + column * part[:each].astype(F32)
        return result, top, total

    def merge_tile(u):
        h, _, tile = unit(u)
        await_scattered(u)
        result, top, total = mix([nbuf[u, place] for place in range(tile_pairs)])
        hbuf[h, tile, :each] = result.astype(BF16)
        hbuf[h, tile, each:] = stats_rows(top, total)
        remote(hbuf.at[h, tile], fbuf.at[h, my_tile], far_send.at[0], far_recv.at[h], partner(tile)).start()

    def send_direct(d):
        u = merged + d
        for c in range(2):
            stats = obuf[u, c, HEAD_SIZE:]
            top, total = stats[:1], stats[SUM_ROW:SUM_ROW + 1]
            out = (obuf[u, c, :HEAD_SIZE] * (1.0 / total)).T.astype(BF16)
            dbuf[d, c, :, :each] = out.reshape(tile_pairs, each, HEAD_SIZE)
            stats = stats_rows(top, total)
            for place in range(tile_pairs):
                dbuf[d, c, place, each:] = stats
        for j, other in others:
            place = lax.rem(my_place + j, tile_pairs)
            there = core if other == 0 else 1 - core
            remote(
                dbuf.at[d, there, place], lbuf.at[d, core, my_place], d_send.at[0], d_recv.at[d], neighbour(j, other)
            ).start()
        lbuf[d, core, my_place] = dbuf[d, core, my_place]

    def direct_bytes(count):
        return sbuf.at[pl.ds(0, count), 0]

    def combine(h, d=None):
        if d is None:
            u = near_unit(h)
            await_scattered(u)
            parts = [nbuf[u, place] for place in range(tile_pairs)]
        else:
            await_bytes(direct_bytes(len(others)), d_recv.at[d])
            parts = [lbuf[d, c, place] for c in range(2) for place in range(tile_pairs)]
        if tiles > 1:
            await_bytes(fbuf.at[h, pl.ds(0, tiles - 1)], far_recv.at[h])
        for step in range(1, tiles):
            parts.append(fbuf[h, lax.rem(my_tile + step, tiles)])
        result, _, _ = mix(parts)
        for g in range(group):
            columns = pl.ds(pl.multiple_of((h * group + g) * HEAD_SIZE, HEAD_SIZE), HEAD_SIZE)
            out_ref[:, columns] = result[g * own:(g + 1) * own].astype(out_ref.dtype)

    def body(u, peeled=LAG):
        h, _, tile = unit(u)
        await_queries(u, peeled)

        for n in {0: (2,), 1: (3, 4), 2: range(5, heads)}.get(peeled, ()):
            if n < heads:
                k_copy(n).start()
                v_copy(n).start()

        if peeled == LAG:
            exchange_copy(u - LAG).wait_recv()
        for v in {1: (4, 5), 2: range(6, late)}.get(peeled, ()):
            if early <= v < late:
                far_head, _, far_tile = unit(jnp.int32(v))
                await_block(far_head, far_tile)
                forward(far_head, far_tile)

        @pl.when(u + 1 < units)
        def _():
            next_head, _, next_tile = unit(u + 1)
            relay(next_head, next_tile)

        if peeled == LAG:

            @pl.when(is_far(u - 2 * LAG))
            def _():
                merge_tile(u - 2 * LAG)

        if peeled == 0:
            segment(None, (h, tile, 0))
        else:
            segment((unit(u - 1)[0], blocks - 1), (h, tile, 0), finish=u - 1)
        for b in range(1, blocks):
            segment((h, b - 1), (h, tile, b))
            if b == 1 and peeled == LAG:
                merge_cores(u - LAG)
        if peeled > 0:

            @pl.when(u - 1 < merged)
            def _():
                exchange_copy(u - 1).start()

        if peeled == LAG:
            scatter(u - LAG)

    pl.semaphore_wait(barrier, tile_devices - 1 + my_tile)
    for h in range(heads):
        await_block(h, my_tile)
    for h in range(early):
        if h == 0:
            forward_to_all(h)
        else:
            forward(h, my_tile)
    lax.fori_loop(0, my_tile, lambda t, _: (signal(ready, partner(t)), 0)[1], 0)

    @pl.when(my_tile < tiles - 1)
    def _():
        pl.semaphore_wait(ready, tiles - 1 - my_tile)

    for step in range(1, tiles):
        tile = lax.rem(my_tile + step, tiles)
        for h in range(heads):
            mine = qbuf.at[h, my_tile, core, my_place]
            remote(mine, mine, far_query_send.at[0], block_recv.at[h, my_tile], partner(tile)).start()
    for h in range(early, heads):
        forward(h, my_tile)
    for u in range(early, min(4, late)):
        far_head, _, far_tile = unit(jnp.int32(u))
        await_block(far_head, far_tile)
        forward(far_head, far_tile)
    if heads > 1:
        k_copy(1).start()
        v_copy(1).start()
    if early == 0:
        first_head, _, first_tile = unit(jnp.int32(0))
        relay(first_head, first_tile)
    fk_copy.wait()
    fv_copy.wait()
    for u in range(min(LAG, units)):
        body(jnp.int32(u), u)
    lax.fori_loop(LAG, units, lambda u, _: (body(u), 0)[1], 0)

    def drain():
        forwards = units * (tile_pairs - 1) + (tile_pairs if early > 0 else 0)
        relays = (units - 1 if early > 0 else units) * tile_pairs
        await_bytes(kbuf.at[0, pl.ds(0, relays * each)], relay_send.at[0])
        await_bytes(kbuf.at[0, pl.ds(0, forwards * each)], gather_send.at[0])
        if merged > 0:
            await_bytes(xbuf.at[pl.ds(0, merged)], x_send.at[0])
            await_bytes(nbuf.at[pl.ds(0, merged), pl.ds(0, tile_pairs - 1)], n_send.at[0])
        if tiles > 1:
            await_bytes(qbuf.at[:, pl.ds(0, tiles - 1), 0, 0], far_query_send.at[0])
            await_bytes(fbuf.at[:, pl.ds(0, tiles - 1)], far_send.at[0])
        for d in range(direct):
            await_bytes(direct_bytes(len(others)), d_send.at[0])

    def merge_and_scatter(u):
        exchange_copy(u).wait_recv()
        merge_cores(u)
        scatter(u)

    last = units - 1
    if direct > 1:
        send_direct(0)
    segment((unit(jnp.int32(last))[0], blocks - 1), None, finish=last)
    send_direct(direct - 1)
    for u in range(max(0, units - LAG), merged):
        merge_and_scatter(u)
    for u in range(max(early, units - 2 * LAG), late):
        merge_tile(jnp.int32(u))
    lax.fori_loop(0, heads - direct, lambda h, _: (combine(h), 0)[1], 0)
    drain()
    for d in range(direct):
        combine(heads - direct + d, d)


def solution(mesh):
    devices = mesh.shape["ctx"]

    def shards(queries, cache_keys, prefix_values, incoming_keys, incoming_values):
        own = queries.shape[0]
        heads = cache_keys.shape[1] // HEAD_SIZE
        group = queries.shape[1] // cache_keys.shape[1]
        depth = cache_keys.shape[0]
        each = group * own
        pairs = devices // 2
        tile_pairs = min(pairs, TILE_ROWS // (2 * each))
        tiles = pairs // tile_pairs
        rows = 2 * tile_pairs * each
        units = heads * tiles
        block = min(BLOCK_KEYS, depth // 2)
        dma = pltpu.SemaphoreType.DMA
        return pl.pallas_call(
            functools.partial(kernel, devices, heads, group, own, block),
            out_shape=jax.ShapeDtypeStruct(queries.shape, queries.dtype),
            in_specs=[pl.BlockSpec(memory_space=pl.ANY)] * 5,
            out_specs=pl.BlockSpec(memory_space=pltpu.VMEM),
            scratch_shapes=[
                pltpu.VMEM((heads, tiles, 2, tile_pairs, each, HEAD_SIZE), BF16),
                pltpu.VMEM((heads, depth, HEAD_SIZE), BF16),
                pltpu.VMEM((heads, depth, HEAD_SIZE), BF16),
                pltpu.VMEM((own, heads * HEAD_SIZE), BF16),
                pltpu.VMEM((own, heads * HEAD_SIZE), BF16),
                pltpu.VMEM((block, rows), F32),
                pltpu.VMEM((block, rows), F32),
                pltpu.VMEM((own, rows), F32),
                pltpu.VMEM((own, rows), jnp.int32),
                pltpu.VMEM((2, SUBLANES, rows), F32),
                pltpu.VMEM((SUBLANES, rows), F32),
                pltpu.VMEM((HEAD_SIZE + SUM_ROWS, rows), F32),
                pltpu.VMEM((units, 2, HEAD_SIZE + SUBLANES, rows // 2), F32),
                pltpu.VMEM((units, HEAD_SIZE + SUBLANES, rows // 2), F32),
                pltpu.VMEM((units, tile_pairs, each + STAT_ROWS, HEAD_SIZE), BF16),
                pltpu.VMEM((units, tile_pairs, each + STAT_ROWS, HEAD_SIZE), BF16),
                pltpu.VMEM((heads, tiles, each + STAT_ROWS, HEAD_SIZE), BF16),
                pltpu.VMEM((heads, tiles, each + STAT_ROWS, HEAD_SIZE), BF16),
                pltpu.VMEM((2, 2, tile_pairs, each + STAT_ROWS, HEAD_SIZE), BF16),
                pltpu.VMEM((2, 2, tile_pairs, each + STAT_ROWS, HEAD_SIZE), BF16),
                dma((heads,)), dma((heads,)), dma((2,)), pltpu.SemaphoreType.REGULAR,
                dma((heads, tiles)), dma((heads, tiles)), dma((heads, tiles)),
                dma((units,)), dma((units,)), dma((heads,)), dma((2,)),
                *[dma((1,))] * 7,
            ],
            compiler_params=pltpu.CompilerParams(
                collective_id=0, has_side_effects=True, vmem_limit_bytes=60 * 1024 * 1024
            ),
        )(queries, cache_keys, prefix_values, incoming_keys, incoming_values)

    spec = P("ctx", "head")
    return jax.shard_map(
        shards, mesh=mesh, in_specs=(spec,) * 5, out_specs=spec, check_vma=False
    )
```

```python
import functools
import math

import jax
import jax.numpy as jnp
from jax import lax
from jax.experimental import pallas as pl
from jax.experimental.pallas import tpu as pltpu
from jax.sharding import PartitionSpec as P

HEAD_SIZE = 128
LANES = 128
SUBLANES = 8
SUM_ROW = 4
STAT_ROWS = 16
SUM_ROWS = 16
LAG = 3
TILE_ROWS = 256
BLOCK_KEYS = 2048
PIECE_KEYS = 256
EXP2_SCALE = 168.0 ** (-0.5) * math.log2(math.e)
MASKED = -1e30
BF16, F32 = jnp.bfloat16, jnp.float32


def nt_dot(a, b):
    return lax.dot_general(a, b, (((1,), (1,)), ((), ())), preferred_element_type=F32)


def weigh(values, weights):
    ones = jnp.ones((SUM_ROWS, values.shape[0]), BF16)
    return jnp.dot(jnp.concatenate([values.T, ones], axis=0), weights, preferred_element_type=F32)


def stats_rows(top, total):
    rows, parts = lax.broadcasted_iota(jnp.int32, (STAT_ROWS, top.shape[1]), 0), []
    for value in (top, total):
        high = value.astype(BF16).astype(F32)
        middle = (value - high).astype(BF16).astype(F32)
        parts += [high, middle, value - high - middle]
    out = jnp.zeros(rows.shape, F32)
    for i, part in enumerate(parts):
        out = jnp.where(rows == i, part, out)
    return out.astype(BF16)


def read_stats(rows):
    x = rows.astype(F32)
    return x[0:1] + x[1:2] + x[2:3], x[3:4] + x[4:5] + x[5:6]


def fold(x, op):
    parts = [x[i] for i in range(x.shape[0])]
    while len(parts) > 1:
        parts = [op(*parts[i:i + 2]) if i + 1 < len(parts) else parts[i] for i in range(0, len(parts), 2)]
    return parts[0]


def kernel(
    devices, heads, group, own, block,
    q_hbm, k_hbm, v_hbm, fk_hbm, fv_hbm, out_ref,
    qbuf, kbuf, vbuf, fkbuf, fvbuf, scores_even, scores_odd, fresh_scores, relative,
    block_max, row_max, acc, obuf, xbuf, sbuf, nbuf, hbuf, fbuf, dbuf, lbuf,
    k_sem, v_sem, f_sem, ready, block_recv, gather_recv, relay_recv, x_recv, n_recv, far_recv, d_recv,
    far_query_send, gather_send, relay_send, x_send, n_send, far_send, d_send,
):
    tiles, tile_pairs = qbuf.shape[1], qbuf.shape[3]
    each = group * own
    half = tile_pairs * each
    rows = 2 * half
    tile_devices = 2 * tile_pairs
    blocks = kbuf.shape[1] // block
    units = heads * tiles
    early = heads // 2 if tiles > 1 else heads
    late = early + heads * (tiles - 1)
    direct = min(2, heads - early if tiles > 1 else heads)
    merged = units - direct
    me = lax.axis_index("ctx")
    core, pair = lax.rem(me, 2), lax.div(me, 2)
    my_tile, my_place = lax.div(pair, tile_pairs), lax.rem(pair, tile_pairs)

    def is_far(u):
        return (u >= early) & (u < late)

    def unit(u):
        far = jnp.maximum(u - early, 0)
        near = jnp.where(u < early, u, u - heads * (tiles - 1))
        h = jnp.where(is_far(u), lax.rem(far, heads), near)
        step = jnp.where(is_far(u), 1 + lax.div(far, heads), 0)
        return h, step, lax.rem(my_tile + step, tiles)

    def near_unit(h):
        return jnp.where(h < early, h, h + heads * (tiles - 1))

    def neighbour(j, other=0):
        there = core if other == 0 else 1 - core
        return {"ctx": (my_tile * tile_pairs + lax.rem(my_place + j, tile_pairs)) * 2 + there}

    others = [(j, other) for j in range(tile_pairs - 1, -1, -1) for other in range(2) if j + other > 0]

    sibling = {"ctx": pair * 2 + 1 - core}

    def partner(tile):
        return {"ctx": (tile * tile_pairs + my_place) * 2 + core}

    def remote(src, dst, send_sem, recv_sem, device):
        return pltpu.make_async_remote_copy(
            src_ref=src, dst_ref=dst, send_sem=send_sem, recv_sem=recv_sem,
            device_id=device, device_id_type=pl.DeviceIdType.MESH,
        )

    def await_bytes(ref, sem):
        pltpu.make_async_copy(ref, ref, sem).wait()

    def head_columns(h):
        return pl.ds(pl.multiple_of(h * HEAD_SIZE, HEAD_SIZE), HEAD_SIZE)

    def k_copy(h):
        return pltpu.make_async_copy(k_hbm.at[:, head_columns(h)], kbuf.at[h], k_sem.at[h])

    def v_copy(h):
        return pltpu.make_async_copy(v_hbm.at[:, head_columns(h)], vbuf.at[h], v_sem.at[h])

    fk_copy = pltpu.make_async_copy(fk_hbm, fkbuf, f_sem.at[0])
    fv_copy = pltpu.make_async_copy(fv_hbm, fvbuf, f_sem.at[1])

    barrier = pltpu.get_barrier_semaphore()

    def signal(sem, device):
        pl.semaphore_signal(sem, inc=1, device_id=device, device_id_type=pl.DeviceIdType.MESH)

    def load_queries(h):
        for g in range(group):
            columns = pl.ds((h * group + g) * HEAD_SIZE, HEAD_SIZE)
            pltpu.make_async_copy(
                q_hbm.at[:, columns], qbuf.at[h, my_tile, core, my_place, pl.ds(g * own, own)],
                block_recv.at[h, my_tile],
            ).start()

    load_queries(0)
    for j in range(1, tile_devices):
        signal(barrier, {"ctx": my_tile * tile_devices + lax.rem(lax.rem(me, tile_devices) + j, tile_devices)})
    lax.fori_loop(my_tile + 1, tiles, lambda t, _: (signal(barrier, partner(t)), 0)[1], 0)

    for h in range(1, heads):
        load_queries(h)
    k_copy(0).start()
    fk_copy.start()
    fv_copy.start()
    v_copy(0).start()

    row = lax.broadcasted_iota(jnp.int32, (own, rows), 1)
    key = lax.broadcasted_iota(jnp.int32, (own, rows), 0)
    device = lax.div(lax.rem(row, half), each) * 2 + lax.div(row, half)
    relative[...] = device * own + lax.rem(row, own) - key

    def await_block(h, tile):
        await_bytes(qbuf.at[h, tile, core, my_place], block_recv.at[h, tile])

    def forward(h, tile):
        mine = qbuf.at[h, tile, core, my_place]
        for j in range(1, tile_pairs):
            remote(mine, mine, gather_send.at[0], gather_recv.at[h, tile], neighbour(j)).start()

    def forward_to_all(h):
        mine = qbuf.at[h, my_tile, core, my_place]
        for j, other in others:
            remote(mine, mine, gather_send.at[0], gather_recv.at[h, my_tile], neighbour(j, other)).start()

    def await_all(h):
        await_bytes(sbuf.at[pl.ds(0, len(others)), 0, pl.ds(0, each)], gather_recv.at[h, my_tile])

    def relay_copy(h, tile):
        mine = qbuf.at[h, tile, core]
        return remote(mine, mine, relay_send.at[0], relay_recv.at[h, tile], sibling)

    def relay(h, tile):
        await_bytes(qbuf.at[h, tile, core, pl.ds(0, tile_pairs - 1)], gather_recv.at[h, tile])
        relay_copy(h, tile).start()

    def await_queries(u, peeled):
        h, step, tile = unit(u)
        if peeled == 0 and early > 0:
            await_all(0)
        else:
            relay_copy(h, tile).wait_recv()

        @pl.when((u < early) | ((step == 1) & (h >= early)))
        def _():
            k_copy(h).wait()
            v_copy(h).wait()

    score_slots = (scores_even, scores_odd)

    def score_piece(h, queries, b, j):
        keys = kbuf[h, pl.ds(b * block + j * PIECE_KEYS, PIECE_KEYS), :]
        s = nt_dot(keys, queries)
        score_slots[b % 2][pl.ds(j * PIECE_KEYS, PIECE_KEYS), :] = s
        return fold(s.reshape(PIECE_KEYS // SUBLANES, SUBLANES, rows), jnp.maximum)

    def score_fresh(h, tile, queries):
        s = nt_dot(fkbuf[:, head_columns(h)], queries)
        seen = relative[...] >= (me - tile * tile_devices) * own
        s = jnp.where(seen, s, MASKED)
        fresh_scores[...] = s
        return fold(s.reshape(own // SUBLANES, SUBLANES, rows), jnp.maximum)

    def segment(values, scores, finish=None):
        if values is not None:
            vh, vb = values
            top = jnp.max(block_max[vb % 2], axis=0, keepdims=True)
            if vb > 0:
                before = row_max[0:1]
                top = jnp.maximum(before, top)
                decay = jnp.exp2((before - top) * EXP2_SCALE)
            row_max[0:1] = top
            top8 = jnp.broadcast_to(top, (SUBLANES, rows))
            weights = []
        if scores is not None:
            sh, tile, sb = scores
            queries = qbuf[sh, tile].reshape(rows, HEAD_SIZE)
            tops = []
        for j in range(block // PIECE_KEYS):
            if values is not None:
                s = score_slots[vb % 2][pl.ds(j * PIECE_KEYS, PIECE_KEYS), :]
                s = s.reshape(PIECE_KEYS // SUBLANES, SUBLANES, rows)
                p = jnp.exp2((s - top8[None]) * EXP2_SCALE)
                weights.append(p.reshape(PIECE_KEYS, rows).astype(BF16))
            if scores is not None:
                tops.append(score_piece(sh, queries, sb, j))
        if scores is not None:
            if sb == 0:
                tops.append(score_fresh(sh, tile, queries))
            block_max[sb % 2] = functools.reduce(jnp.maximum, tops)
        if values is not None:
            out = weigh(vbuf[vh, pl.ds(vb * block, block), :], jnp.concatenate(weights, axis=0))
            if vb == 0:
                s = fresh_scores[...].reshape(own // SUBLANES, SUBLANES, rows)
                p = jnp.exp2((s - top8[None]) * EXP2_SCALE)
                out = out + weigh(fvbuf[:, head_columns(vh)], p.reshape(own, rows).astype(BF16))
            if vb > 0:
                out = acc[...] * decay + out
            if finish is None:
                acc[...] = out
            else:
                total = out[HEAD_SIZE:HEAD_SIZE + 1]
                out = out[:HEAD_SIZE]
                upper = lax.broadcasted_iota(jnp.int32, (SUBLANES, half), 0) < SUM_ROW
                for c in range(2):
                    span = slice(c * half, (c + 1) * half)
                    obuf[finish, c, :HEAD_SIZE] = out[:, span]
                    obuf[finish, c, HEAD_SIZE:] = jnp.where(upper, top[:, span], total[:, span])

    def exchange_copy(u):
        return remote(obuf.at[u, 1 - core], xbuf.at[u], x_send.at[0], x_recv.at[u], sibling)

    def merge_cores(u):
        own_part, other_part = obuf[u, core, HEAD_SIZE:], xbuf[u, HEAD_SIZE:]
        top_a, top_b = own_part[:1], other_part[:1]
        sum_a, sum_b = own_part[SUM_ROW:SUM_ROW + 1], other_part[SUM_ROW:SUM_ROW + 1]
        top = jnp.maximum(top_a, top_b)
        scale_a = jnp.exp2((top_a - top) * EXP2_SCALE)
        scale_b = jnp.exp2((top_b - top) * EXP2_SCALE)
        total = sum_a * scale_a + sum_b * scale_b
        out = obuf[u, core, :HEAD_SIZE] * (scale_a / total) + xbuf[u, :HEAD_SIZE] * (scale_b / total)
        sbuf[u, :, :each] = out.T.astype(BF16).reshape(tile_pairs, each, HEAD_SIZE)
        stats = stats_rows(top, total)
        for place in range(tile_pairs):
            sbuf[u, place, each:] = stats
        nbuf[u, my_place] = sbuf[u, my_place]

    def scatter(u):
        for j in range(1, tile_pairs):
            place = lax.rem(my_place + j, tile_pairs)
            remote(sbuf.at[u, place], nbuf.at[u, my_place], n_send.at[0], n_recv.at[u], neighbour(j)).start()

    def await_scattered(u):
        await_bytes(nbuf.at[u, pl.ds(0, tile_pairs - 1)], n_recv.at[u])

    def mix(parts):
        tops, sums = zip(*[read_stats(part[each:]) for part in parts], strict=True)
        tops, sums = jnp.concatenate(tops, axis=0), jnp.concatenate(sums, axis=0)
        top = jnp.max(tops, axis=0, keepdims=True)
        weights = jnp.exp2((tops - top) * EXP2_SCALE) * sums
        total = jnp.sum(weights, axis=0, keepdims=True)
        weights = weights / total
        mine = jnp.zeros((len(parts), each), F32)
        for place in range(tile_pairs):
            mine = jnp.where(my_place == place, weights[:, place * each:(place + 1) * each], mine)
        diagonal = lax.broadcasted_iota(jnp.int32, (each, each), 0) == lax.broadcasted_iota(
            jnp.int32, (each, each), 1
        )
        result = jnp.zeros((each, HEAD_SIZE), F32)
        for source, part in enumerate(parts):
            line = jnp.broadcast_to(mine[source:source + 1, :], (each, each))
            column = jnp.sum(jnp.where(diagonal, line, 0.0), axis=1, keepdims=True)
            result = result + column * part[:each].astype(F32)
        return result, top, total

    def merge_tile(u):
        h, _, tile = unit(u)
        await_scattered(u)
        result, top, total = mix([nbuf[u, place] for place in range(tile_pairs)])
        hbuf[h, tile, :each] = result.astype(BF16)
        hbuf[h, tile, each:] = stats_rows(top, total)
        remote(hbuf.at[h, tile], fbuf.at[h, my_tile], far_send.at[0], far_recv.at[h], partner(tile)).start()

    def send_direct(d):
        u = merged + d
        for c in range(2):
            stats = obuf[u, c, HEAD_SIZE:]
            top, total = stats[:1], stats[SUM_ROW:SUM_ROW + 1]
            out = (obuf[u, c, :HEAD_SIZE] * (1.0 / total)).T.astype(BF16)
            dbuf[d, c, :, :each] = out.reshape(tile_pairs, each, HEAD_SIZE)
            stats = stats_rows(top, total)
            for place in range(tile_pairs):
                dbuf[d, c, place, each:] = stats
        for j, other in others:
            place = lax.rem(my_place + j, tile_pairs)
            there = core if other == 0 else 1 - core
            remote(
                dbuf.at[d, there, place], lbuf.at[d, core, my_place], d_send.at[0], d_recv.at[d], neighbour(j, other)
            ).start()
        lbuf[d, core, my_place] = dbuf[d, core, my_place]

    def direct_bytes(count):
        return sbuf.at[pl.ds(0, count), 0]

    def combine(h, d=None):
        if d is None:
            u = near_unit(h)
            await_scattered(u)
            parts = [nbuf[u, place] for place in range(tile_pairs)]
        else:
            await_bytes(direct_bytes(len(others)), d_recv.at[d])
            parts = [lbuf[d, c, place] for c in range(2) for place in range(tile_pairs)]
        if tiles > 1:
            await_bytes(fbuf.at[h, pl.ds(0, tiles - 1)], far_recv.at[h])
        for step in range(1, tiles):
            parts.append(fbuf[h, lax.rem(my_tile + step, tiles)])
        result, _, _ = mix(parts)
        for g in range(group):
            columns = pl.ds(pl.multiple_of((h * group + g) * HEAD_SIZE, HEAD_SIZE), HEAD_SIZE)
            out_ref[:, columns] = result[g * own:(g + 1) * own].astype(out_ref.dtype)

    def body(u, peeled=LAG):
        h, _, tile = unit(u)
        await_queries(u, peeled)

        for n in {0: (2,), 1: (3, 4), 2: range(5, heads)}.get(peeled, ()):
            if n < heads:
                k_copy(n).start()
                v_copy(n).start()

        if peeled == LAG:
            exchange_copy(u - LAG).wait_recv()
        for v in {1: (4, 5), 2: range(6, late)}.get(peeled, ()):
            if early <= v < late:
                far_head, _, far_tile = unit(jnp.int32(v))
                await_block(far_head, far_tile)
                forward(far_head, far_tile)

        @pl.when(u + 1 < units)
        def _():
            next_head, _, next_tile = unit(u + 1)
            relay(next_head, next_tile)

        if peeled == LAG:

            @pl.when(is_far(u - 2 * LAG))
            def _():
                merge_tile(u - 2 * LAG)

        if peeled == 0:
            segment(None, (h, tile, 0))
        else:
            segment((unit(u - 1)[0], blocks - 1), (h, tile, 0), finish=u - 1)
        for b in range(1, blocks):
            segment((h, b - 1), (h, tile, b))
            if b == 1 and peeled == LAG:
                merge_cores(u - LAG)
        if peeled > 0:

            @pl.when(u - 1 < merged)
            def _():
                exchange_copy(u - 1).start()

        if peeled == LAG:
            scatter(u - LAG)

    pl.semaphore_wait(barrier, tile_devices - 1 + my_tile)
    for h in range(early):
        await_block(h, my_tile)
        if h == 0:
            forward_to_all(h)
        else:
            forward(h, my_tile)
    lax.fori_loop(0, my_tile, lambda t, _: (signal(ready, partner(t)), 0)[1], 0)

    for h in range(early, heads):
        await_block(h, my_tile)

    @pl.when(my_tile < tiles - 1)
    def _():
        pl.semaphore_wait(ready, tiles - 1 - my_tile)

    for step in range(1, tiles):
        tile = lax.rem(my_tile + step, tiles)
        for h in range(heads):
            mine = qbuf.at[h, my_tile, core, my_place]
            remote(mine, mine, far_query_send.at[0], block_recv.at[h, my_tile], partner(tile)).start()
    for h in range(early, heads):
        forward(h, my_tile)
    for u in range(early, min(4, late)):
        far_head, _, far_tile = unit(jnp.int32(u))
        await_block(far_head, far_tile)
        forward(far_head, far_tile)
    if heads > 1:
        k_copy(1).start()
        v_copy(1).start()
    if early == 0:
        first_head, _, first_tile = unit(jnp.int32(0))
        relay(first_head, first_tile)
    fk_copy.wait()
    fv_copy.wait()
    for u in range(min(LAG, units)):
        body(jnp.int32(u), u)
    lax.fori_loop(LAG, units, lambda u, _: (body(u), 0)[1], 0)

    def drain():
        forwards = units * (tile_pairs - 1) + (tile_pairs if early > 0 else 0)
        relays = (units - 1 if early > 0 else units) * tile_pairs
        await_bytes(kbuf.at[0, pl.ds(0, relays * each)], relay_send.at[0])
        await_bytes(kbuf.at[0, pl.ds(0, forwards * each)], gather_send.at[0])
        if merged > 0:
            await_bytes(xbuf.at[pl.ds(0, merged)], x_send.at[0])
            await_bytes(nbuf.at[pl.ds(0, merged), pl.ds(0, tile_pairs - 1)], n_send.at[0])
        if tiles > 1:
            await_bytes(qbuf.at[:, pl.ds(0, tiles - 1), 0, 0], far_query_send.at[0])
            await_bytes(fbuf.at[:, pl.ds(0, tiles - 1)], far_send.at[0])
        for d in range(direct):
            await_bytes(direct_bytes(len(others)), d_send.at[0])

    def merge_and_scatter(u):
        exchange_copy(u).wait_recv()
        merge_cores(u)
        scatter(u)

    last = units - 1
    if direct > 1:
        send_direct(0)
    segment((unit(jnp.int32(last))[0], blocks - 1), None, finish=last)
    send_direct(direct - 1)
    for u in range(max(0, units - LAG), merged):
        merge_and_scatter(u)
    for u in range(max(early, units - 2 * LAG), late):
        merge_tile(jnp.int32(u))
    lax.fori_loop(0, heads - direct, lambda h, _: (combine(h), 0)[1], 0)
    drain()
    for d in range(direct):
        combine(heads - direct + d, d)


def solution(mesh):
    devices = mesh.shape["ctx"]

    def shards(queries, cache_keys, prefix_values, incoming_keys, incoming_values):
        own = queries.shape[0]
        heads = cache_keys.shape[1] // HEAD_SIZE
        group = queries.shape[1] // cache_keys.shape[1]
        depth = cache_keys.shape[0]
        each = group * own
        pairs = devices // 2
        tile_pairs = min(pairs, TILE_ROWS // (2 * each))
        tiles = pairs // tile_pairs
        rows = 2 * tile_pairs * each
        units = heads * tiles
        block = min(BLOCK_KEYS, depth // 2)
        dma = pltpu.SemaphoreType.DMA
        return pl.pallas_call(
            functools.partial(kernel, devices, heads, group, own, block),
            out_shape=jax.ShapeDtypeStruct(queries.shape, queries.dtype),
            in_specs=[pl.BlockSpec(memory_space=pl.ANY)] * 5,
            out_specs=pl.BlockSpec(memory_space=pltpu.VMEM),
            scratch_shapes=[
                pltpu.VMEM((heads, tiles, 2, tile_pairs, each, HEAD_SIZE), BF16),
                pltpu.VMEM((heads, depth, HEAD_SIZE), BF16),
                pltpu.VMEM((heads, depth, HEAD_SIZE), BF16),
                pltpu.VMEM((own, heads * HEAD_SIZE), BF16),
                pltpu.VMEM((own, heads * HEAD_SIZE), BF16),
                pltpu.VMEM((block, rows), F32),
                pltpu.VMEM((block, rows), F32),
                pltpu.VMEM((own, rows), F32),
                pltpu.VMEM((own, rows), jnp.int32),
                pltpu.VMEM((2, SUBLANES, rows), F32),
                pltpu.VMEM((SUBLANES, rows), F32),
                pltpu.VMEM((HEAD_SIZE + SUM_ROWS, rows), F32),
                pltpu.VMEM((units, 2, HEAD_SIZE + SUBLANES, rows // 2), F32),
                pltpu.VMEM((units, HEAD_SIZE + SUBLANES, rows // 2), F32),
                pltpu.VMEM((units, tile_pairs, each + STAT_ROWS, HEAD_SIZE), BF16),
                pltpu.VMEM((units, tile_pairs, each + STAT_ROWS, HEAD_SIZE), BF16),
                pltpu.VMEM((heads, tiles, each + STAT_ROWS, HEAD_SIZE), BF16),
                pltpu.VMEM((heads, tiles, each + STAT_ROWS, HEAD_SIZE), BF16),
                pltpu.VMEM((2, 2, tile_pairs, each + STAT_ROWS, HEAD_SIZE), BF16),
                pltpu.VMEM((2, 2, tile_pairs, each + STAT_ROWS, HEAD_SIZE), BF16),
                dma((heads,)), dma((heads,)), dma((2,)), pltpu.SemaphoreType.REGULAR,
                dma((heads, tiles)), dma((heads, tiles)), dma((heads, tiles)),
                dma((units,)), dma((units,)), dma((heads,)), dma((2,)),
                *[dma((1,))] * 7,
            ],
            compiler_params=pltpu.CompilerParams(
                collective_id=0, has_side_effects=True, vmem_limit_bytes=60 * 1024 * 1024
            ),
        )(queries, cache_keys, prefix_values, incoming_keys, incoming_values)

    spec = P("ctx", "head")
    return jax.shard_map(
        shards, mesh=mesh, in_specs=(spec,) * 5, out_specs=spec, check_vma=False
    )
```
